32 devices in a mesh: gx: 16 (over z, x, core), ta: 2 (over y).
Axes of the slice: x: 2, y: 2, z: 4, core: 2. Of those that a mesh axis runs over, the one named last changes fastest.
Arguments:
- master_flat: float32 [8388608], P(('gx', 'ta')), may hold values from -6 to 6
Outputs:
- serving_weight: bfloat16 [1, 8192, 1024], P(None, None, 'ta')
- channel_scale: float32 [1, 1024], P(None, 'ta')
The draws below stay inside these ranges and needn't reach their ends.
All inputs are finite; a program needn't handle non-finite values.
Results may differ from the reference program's by a relative error of at most 0.015.
Values may be sent and summed in bfloat16 or wider, within the bound.
A program may use at most 64 MiB of HBM per device.

```python
import jax
import jax.numpy as jnp

D = 8192
KVH = 8
HEAD = 128
LAYERS = 1


def level_of(own_key, dims, split, least, top_value):
    factor_of, own = 1.0, jax.random.fold_in(own_key, 6)
    for axis_at, blocks in split:
        steps = jnp.exp(jax.random.uniform(jax.random.fold_in(own, axis_at), (blocks,), jnp.float32, least / len(split), top_value / len(split)))
        factor_of = factor_of * jnp.repeat(steps, dims[axis_at] // blocks).reshape([-1 if axis == axis_at else 1 for axis in range(len(dims))])
    return factor_of


def gaussian(key, shape, deviation, bound, cuts=(), kind=jnp.bfloat16):
    level = level_of(key, shape, cuts, -0.22, 0.18) if cuts else 1.0
    values = jax.random.normal(key, shape, jnp.float32) * deviation * level
    return jnp.minimum(jnp.maximum(values, -bound), bound).astype(kind)


def setup_inputs(seed: int = 0) -> dict:
    seeds = jax.random.split(jax.random.key(seed), 2)
    return {
        "master_flat": gaussian(seeds[0], (LAYERS * D * KVH * HEAD,), 1.0, 6.0, ((0, 32),), jnp.float32),
    }


def reference(master_flat):
    weight = master_flat.reshape(LAYERS, D, KVH * HEAD).astype(jnp.bfloat16)
    wide = weight.astype(jnp.float32)
    channel_scale = jnp.max(jnp.abs(wide), axis=1)
    serving_weight = (wide / channel_scale[:, None, :]).astype(jnp.bfloat16)
    return serving_weight, channel_scale
```

```python
import functools

import jax
import jax.numpy as jnp
from jax import lax
from jax.experimental import pallas as pl
from jax.experimental.pallas import tpu as pltpu
from jax.sharding import PartitionSpec as P

D = 8192
KVH = 8
HEAD = 128
LAYERS = 1
LANES = 128
CORES = 2
MESH = pl.DeviceIdType.MESH


def ring_order(mesh, chips):
    where = [getattr(d, "coords", None) for d in mesh.devices[::CORES, 0]]
    wide = 1
    if all(w is not None for w in where) and chips > 2:
        moved = [a != b for a, b in zip(where[0], where[1])].index(True)
        wide = next((c for c in range(1, chips) if where[c][moved] == where[0][moved]), chips)
    tall = chips // wide
    if wide == 1 or wide == chips or tall % 2:
        return list(range(chips))
    order = [0]
    for a in range(tall):
        columns = range(1, wide) if a % 2 == 0 else range(wide - 1, 0, -1)
        order += [a * wide + b for b in columns]
    return order + [a * wide for a in range(tall - 1, 0, -1)]


def pick(table, index):
    found = jnp.int32(table[0])
    for at in range(1, len(table)):
        found = jnp.where(index == at, jnp.int32(table[at]), found)
    return found


def kernel(n, t, order, splits, x_ref, out_ref, scale_ref,
           gath, loc, top, tops, cw_send, cw_recv, cc_send, cc_recv, dd_send, dd_recv,
           ta_send, ta_recv, top_send, top_recv):
    chips = n // CORES
    rows, width = gath.shape
    blocks = width // LANES
    piece = loc.shape[1]
    unit = piece * t
    chunk = piece // splits
    count = t * splits
    lines = t * blocks
    total = n * t

    gx, ta = lax.axis_index("gx"), lax.axis_index("ta")
    me = gx * t + ta
    chip, core = gx // CORES, lax.rem(gx, CORES)
    place = [order.index(c) for c in range(chips)]
    at = pick(place, chip)

    barrier = pltpu.get_barrier_semaphore()

    def greet(k, carry):
        other = lax.rem(me + k, total)
        pl.semaphore_signal(barrier, inc=1, device_id=(other // t, lax.rem(other, t)), device_id_type=MESH)
        return carry

    lax.fori_loop(1, total, greet, 0)

    best = None
    for r in range(lines):
        block = x_ref[pl.ds(r, piece, stride=lines), :].astype(jnp.bfloat16)
        loc[r // blocks, :, (r % blocks) * LANES:(r % blocks + 1) * LANES] = block
        high = jnp.max(jnp.abs(block.astype(jnp.float32)), axis=0, keepdims=True)
        top[r // blocks, r % blocks:r % blocks + 1, :] = high

    ring = {
        1: (cw_send, cw_recv, pick(order, lax.rem(at + 1, chips))),
        -1: (cc_send, cc_recv, pick(order, lax.rem(at + chips - 1, chips))),
    }
    reach = {
        1: [chips // 2 if j < count // 2 else chips - 1 - chips // 2 for j in range(count)],
        -1: [chips - 1 - chips // 2 if j < count // 2 else chips // 2 for j in range(count)],
    }

    def start_of(chip_at, of_core, j):
        inner = lax.rem(ta * piece + j * chunk, unit)
        return pl.multiple_of((chip_at * CORES + of_core) * unit + inner, chunk)

    def source(hop, start, j):
        if hop == 0 and j < splits:
            return loc.at[ta, pl.ds(j * chunk, chunk), :]
        return gath.at[pl.ds(start, chunk), :]

    started = []

    def send(src, start, send_sem, recv_sem, device):
        copy = pltpu.make_async_remote_copy(
            src_ref=src, dst_ref=gath.at[pl.ds(start, chunk), :], send_sem=send_sem, recv_sem=recv_sem,
            device_id=device, device_id_type=MESH)
        copy.start()
        started.append(copy)

    def arrived(start, sem):
        here = gath.at[pl.ds(start, chunk), :]
        pltpu.make_async_copy(here, here, sem).wait()

    def slot(hop, j):
        return hop * count + j

    def onward(way, hop, j, start):
        if hop < reach[way][j]:
            send_sem, recv_sem, to = ring[way]
            send(source(hop, start, j), start, send_sem.at[slot(hop, j)], recv_sem.at[slot(hop, j)],
                 (to * CORES + core, ta))

    def across(way, hop, j, start):
        index = slot(hop if way > 0 else hop + chips // 2, j)
        send(source(hop, start, j), start, dd_send.at[index], dd_recv.at[index], (chip * CORES + 1 - core, ta))

    pl.semaphore_wait(barrier, total - 1)

    def tell(k, carry):
        other = lax.rem(me + k, total)
        to = lax.rem(other, t)
        pltpu.make_async_remote_copy(
            src_ref=top.at[to], dst_ref=tops.at[k - 1], send_sem=top_send, recv_sem=top_recv,
            device_id=(other // t, to), device_id_type=MESH).start()
        return carry

    lax.fori_loop(1, total, tell, 0)

    for j in range(splits):
        start = start_of(chip, core, j)
        onward(1, 0, j, start)
        onward(-1, 0, j, start)
        for k in range(1, t):
            to = lax.rem(ta + k, t)
            index = (t - k) * splits + j
            send(loc.at[to, pl.ds(j * chunk, chunk), :], start, ta_send.at[index], ta_recv.at[index], (gx, to))
    for j in range(splits):
        across(1, 0, j, start_of(chip, core, j))

    inverse = {}

    def finish(start, own_at=None):
        for_rows = chunk
        step = min(for_rows, 32)

        def some(i, carry):
            for b in range(blocks):
                lanes = slice(b * LANES, (b + 1) * LANES)
                if own_at is None:
                    value = gath[pl.ds(pl.multiple_of(start + i * step, step), step), lanes]
                else:
                    value = loc[ta, pl.ds(pl.multiple_of(own_at + i * step, step), step), lanes]
                out_ref[pl.ds(pl.multiple_of(start + i * step, step), step), lanes] = (
                    value.astype(jnp.float32) / inverse["scale"][b:b + 1, :]).astype(jnp.bfloat16)
            return carry

        lax.fori_loop(0, for_rows // step, some, 0)

    waiting = []
    peer = []

    def settle_peer(keep):
        while len(peer) > keep:
            start, index = peer.pop(0)
            arrived(start, dd_recv.at[index])
            waiting.append((start, None))

    def settle():
        if not inverse:
            return
        while waiting:
            finish(*waiting.pop(0))

    def scale():
        everyone = tops.at[pl.ds(0, total - 1)]
        pltpu.make_async_copy(everyone, everyone, top_recv).wait()
        high = top[ta]

        def more(k, high):
            return jnp.maximum(high, tops[k])

        high = lax.fori_loop(0, total - 1, more, high)
        for b in range(blocks):
            scale_ref[:, b * LANES:(b + 1) * LANES] = high[b:b + 1, :]
        inverse["scale"] = high

    def note_peer(way, hop, j, chip_at):
        peer.append((start_of(chip_at, 1 - core, j), slot(hop if way > 0 else hop + chips // 2, j)))

    for j in range(splits):
        waiting.append((start_of(chip, core, j), j * chunk))
        note_peer(1, 0, j, chip)
    for j in range(splits, count):
        start = start_of(chip, core, j)
        arrived(start, ta_recv.at[j])
        onward(1, 0, j, start)
        onward(-1, 0, j, start)
        across(1, 0, j, start)
        waiting.append((start, None))
        note_peer(1, 0, j, chip)

    for hop in range(1, chips // 2 + 1):
        left = pick(order, lax.rem(at + chips - hop, chips))
        right = pick(order, lax.rem(at + hop, chips))
        for j in range(count):
            for way, origin in ((1, left), (-1, right)):
                if hop > reach[way][j]:
                    continue
                start = start_of(origin, core, j)
                arrived(start, ring[way][1].at[slot(hop - 1, j)])
                onward(way, hop, j, start)
                across(way, hop, j, start)
                waiting.append((start, None))
                note_peer(way, hop, j, origin)
            if hop == 1 and j == 1:
                scale()
            if inverse:
                settle_peer(4)
                settle()
    if not inverse:
        scale()
    settle_peer(0)
    settle()
    for copy in started:
        copy.wait_send()
    everyone = tops.at[pl.ds(0, total - 1)]
    pltpu.make_async_copy(everyone, everyone, top_send).wait()


def shards(mesh, order, master_flat):
    n, t = mesh.shape["gx"], mesh.shape["ta"]
    kv_width = KVH * HEAD
    piece = master_flat.shape[0] // kv_width
    rows, width = piece * n * t, kv_width // t
    blocks = width // LANES
    splits = 2 if piece % 64 == 0 else 1
    count = t * splits
    chips = n // CORES
    hops = chips // 2 * count
    dma = pltpu.SemaphoreType.DMA
    out, scale = pl.pallas_call(
        functools.partial(kernel, n, t, order, splits),
        out_shape=(jax.ShapeDtypeStruct((rows, width), jnp.bfloat16), jax.ShapeDtypeStruct((1, width), jnp.float32)),
        in_specs=[pl.BlockSpec(memory_space=pltpu.VMEM)],
        out_specs=(pl.BlockSpec(memory_space=pltpu.VMEM), pl.BlockSpec(memory_space=pltpu.VMEM)),
        scratch_shapes=[
            pltpu.VMEM((rows, width), jnp.bfloat16),
            pltpu.VMEM((t, piece, width), jnp.bfloat16),
            pltpu.VMEM((t, blocks, LANES), jnp.float32),
            pltpu.VMEM((n * t, blocks, LANES), jnp.float32),
            dma((hops,)), dma((hops,)), dma((hops,)), dma((hops,)),
            dma((2 * hops + 2 * count,)), dma((2 * hops + 2 * count,)),
            dma((count,)), dma((count,)), dma, dma,
        ],
        compiler_params=pltpu.CompilerParams(
            collective_id=0, has_side_effects=True, vmem_limit_bytes=40 * 1024 * 1024),
    )(master_flat.reshape(piece * kv_width // LANES, LANES))
    return out.reshape(LAYERS, D, -1), scale.reshape(LAYERS, -1)


def solution(mesh):
    order = ring_order(mesh, mesh.shape["gx"] // CORES)
    in_specs = (P(("gx", "ta")),)
    out_specs = (P(None, None, "ta"), P(None, "ta"))
    return jax.shard_map(functools.partial(shards, mesh, order), mesh=mesh, in_specs=in_specs, out_specs=out_specs,
                         check_vma=False)
```

```python
import functools

import jax
import jax.numpy as jnp
from jax import lax
from jax.experimental import pallas as pl
from jax.experimental.pallas import tpu as pltpu
from jax.sharding import PartitionSpec as P

D = 8192
KVH = 8
HEAD = 128
LAYERS = 1
LANES = 128
CORES = 2
PARTS = 8
MESH = pl.DeviceIdType.MESH


def ring_order(mesh, chips):
    where = [getattr(d, "coords", None) for d in mesh.devices[::CORES, 0]]
    wide = 1
    if all(w is not None for w in where) and chips > 2:
        moved = [a != b for a, b in zip(where[0], where[1])].index(True)
        wide = next((c for c in range(1, chips) if where[c][moved] == where[0][moved]), chips)
    tall = chips // wide
    if wide == 1 or wide == chips or tall % 2:
        return list(range(chips))
    order = [0]
    for a in range(tall):
        columns = range(1, wide) if a % 2 == 0 else range(wide - 1, 0, -1)
        order += [a * wide + b for b in columns]
    return order + [a * wide for a in range(tall - 1, 0, -1)]


def pick(table, index):
    found = jnp.int32(table[0])
    for at in range(1, len(table)):
        found = jnp.where(index == at, jnp.int32(table[at]), found)
    return found


def kernel(n, t, order, splits, master_ref, out_ref, scale_ref,
           x_ref, x_sem, gath, loc, top, tops, cw_send, cw_recv, cc_send, cc_recv, dd_send, dd_recv,
           ta_send, ta_recv, top_send, top_recv):
    chips = n // CORES
    rows, width = gath.shape
    blocks = width // LANES
    piece = loc.shape[1]
    unit = piece * t
    chunk = piece // splits
    count = t * splits
    lines = t * blocks
    total = n * t

    gx, ta = lax.axis_index("gx"), lax.axis_index("ta")
    me = gx * t + ta
    chip, core = gx // CORES, lax.rem(gx, CORES)
    place = [order.index(c) for c in range(chips)]
    at = pick(place, chip)

    bring = pltpu.make_async_copy(master_ref, x_ref, x_sem)
    bring.start()
    barrier = pltpu.get_barrier_semaphore()

    def greet(k, carry):
        other = lax.rem(me + k, total)
        pl.semaphore_signal(barrier, inc=1, device_id=(other // t, lax.rem(other, t)), device_id_type=MESH)
        return carry

    lax.fori_loop(1, total, greet, 0)

    bring.wait()
    for r in range(lines):
        block = x_ref[pl.ds(r, piece, stride=lines), :].astype(jnp.bfloat16)
        loc[r // blocks, :, (r % blocks) * LANES:(r % blocks + 1) * LANES] = block
        high = jnp.max(jnp.abs(block.astype(jnp.float32)), axis=0, keepdims=True)
        top[r // blocks, r % blocks:r % blocks + 1, :] = high

    ring = {
        1: (cw_send, cw_recv, pick(order, lax.rem(at + 1, chips))),
        -1: (cc_send, cc_recv, pick(order, lax.rem(at + chips - 1, chips))),
    }
    reach = {
        1: [chips // 2 if j < count // 2 else chips - 1 - chips // 2 for j in range(count)],
        -1: [chips - 1 - chips // 2 if j < count // 2 else chips // 2 for j in range(count)],
    }

    def start_of(chip_at, of_core, j):
        inner = lax.rem(ta * piece + j * chunk, unit)
        return pl.multiple_of((chip_at * CORES + of_core) * unit + inner, chunk)

    def source(hop, start, j):
        if hop == 0 and j < splits:
            return loc.at[ta, pl.ds(j * chunk, chunk), :]
        return gath.at[pl.ds(start, chunk), :]

    started = []

    def send(src, start, send_sem, recv_sem, device):
        copy = pltpu.make_async_remote_copy(
            src_ref=src, dst_ref=gath.at[pl.ds(start, chunk), :], send_sem=send_sem, recv_sem=recv_sem,
            device_id=device, device_id_type=MESH)
        copy.start()
        started.append(copy)

    def arrived(start, sem):
        here = gath.at[pl.ds(start, chunk), :]
        pltpu.make_async_copy(here, here, sem).wait()

    def slot(hop, j):
        return hop * count + j

    def onward(way, hop, j, start):
        if hop < reach[way][j]:
            send_sem, recv_sem, to = ring[way]
            send(source(hop, start, j), start, send_sem.at[slot(hop, j)], recv_sem.at[slot(hop, j)],
                 (to * CORES + core, ta))

    def across(way, hop, j, start):
        index = slot(hop if way > 0 else hop + chips // 2, j)
        send(source(hop, start, j), start, dd_send.at[index], dd_recv.at[index], (chip * CORES + 1 - core, ta))

    pl.semaphore_wait(barrier, total - 1)

    def tell(k, carry):
        other = lax.rem(me + k, total)
        to = lax.rem(other, t)
        pltpu.make_async_remote_copy(
            src_ref=top.at[to], dst_ref=tops.at[k - 1], send_sem=top_send, recv_sem=top_recv,
            device_id=(other // t, to), device_id_type=MESH).start()
        return carry

    lax.fori_loop(1, total, tell, 0)

    for j in range(splits):
        start = start_of(chip, core, j)
        onward(1, 0, j, start)
        onward(-1, 0, j, start)
        for k in range(1, t):
            to = lax.rem(ta + k, t)
            index = (t - k) * splits + j
            send(loc.at[to, pl.ds(j * chunk, chunk), :], start, ta_send.at[index], ta_recv.at[index], (gx, to))
    for j in range(splits):
        across(1, 0, j, start_of(chip, core, j))

    inverse = {}

    def finish(start, own_at=None):
        for_rows = chunk
        step = min(for_rows, 32)

        def some(i, carry):
            for b in range(blocks):
                lanes = slice(b * LANES, (b + 1) * LANES)
                if own_at is None:
                    value = gath[pl.ds(pl.multiple_of(start + i * step, step), step), lanes]
                else:
                    value = loc[ta, pl.ds(pl.multiple_of(own_at + i * step, step), step), lanes]
                out_ref[pl.ds(pl.multiple_of(start + i * step, step), step), lanes] = (
                    value.astype(jnp.float32) / inverse["scale"][b:b + 1, :]).astype(jnp.bfloat16)
            return carry

        lax.fori_loop(0, for_rows // step, some, 0)

    waiting = []
    peer = []

    def settle_peer(keep):
        while len(peer) > keep:
            start, index = peer.pop(0)
            arrived(start, dd_recv.at[index])
            waiting.append((start, None))

    def settle():
        if not inverse:
            return
        while waiting:
            finish(*waiting.pop(0))

    def scale():
        everyone = tops.at[pl.ds(0, total - 1)]
        pltpu.make_async_copy(everyone, everyone, top_recv).wait()
        high = top[ta]

        def more(k, high):
            return jnp.maximum(high, tops[k])

        high = lax.fori_loop(0, total - 1, more, high)
        for b in range(blocks):
            scale_ref[:, b * LANES:(b + 1) * LANES] = high[b:b + 1, :]
        inverse["scale"] = high

    def note_peer(way, hop, j, chip_at):
        peer.append((start_of(chip_at, 1 - core, j), slot(hop if way > 0 else hop + chips // 2, j)))

    for j in range(splits):
        waiting.append((start_of(chip, core, j), j * chunk))
        note_peer(1, 0, j, chip)
    for j in range(splits, count):
        start = start_of(chip, core, j)
        arrived(start, ta_recv.at[j])
        onward(1, 0, j, start)
        onward(-1, 0, j, start)
        across(1, 0, j, start)
        waiting.append((start, None))
        note_peer(1, 0, j, chip)

    for hop in range(1, chips // 2 + 1):
        left = pick(order, lax.rem(at + chips - hop, chips))
        right = pick(order, lax.rem(at + hop, chips))
        for j in range(count):
            for way, origin in ((1, left), (-1, right)):
                if hop > reach[way][j]:
                    continue
                start = start_of(origin, core, j)
                arrived(start, ring[way][1].at[slot(hop - 1, j)])
                onward(way, hop, j, start)
                across(way, hop, j, start)
                waiting.append((start, None))
                note_peer(way, hop, j, origin)
            if hop == 1 and j == 1:
                scale()
            if inverse:
                settle_peer(4)
                settle()
    if not inverse:
        scale()
    settle_peer(0)
    settle()
    for copy in started:
        copy.wait_send()
    everyone = tops.at[pl.ds(0, total - 1)]
    pltpu.make_async_copy(everyone, everyone, top_send).wait()


def store(out_ref, scale_ref, out_hbm, scale_hbm, sems, scale_sem):
    rows = out_ref.shape[0] // PARTS
    copies = [pltpu.make_async_copy(scale_ref, scale_hbm, scale_sem)]
    for i in range(PARTS):
        part = pl.ds(i * rows, rows)
        copies.append(pltpu.make_async_copy(out_ref.at[part, :], out_hbm.at[part, :], sems.at[i]))
    for copy in copies:
        copy.start()
    for copy in copies:
        copy.wait()


def shards(mesh, order, master_flat):
    n, t = mesh.shape["gx"], mesh.shape["ta"]
    kv_width = KVH * HEAD
    piece = master_flat.shape[0] // kv_width
    rows, width = piece * n * t, kv_width // t
    blocks = width // LANES
    splits = 2 if piece % 64 == 0 else 1
    count = t * splits
    chips = n // CORES
    hops = chips // 2 * count
    dma = pltpu.SemaphoreType.DMA
    out, scale = pl.pallas_call(
        functools.partial(kernel, n, t, order, splits),
        out_shape=(jax.ShapeDtypeStruct((rows, width), jnp.bfloat16), jax.ShapeDtypeStruct((1, width), jnp.float32)),
        in_specs=[pl.BlockSpec(memory_space=pltpu.HBM)],
        out_specs=(pl.BlockSpec(memory_space=pltpu.VMEM), pl.BlockSpec(memory_space=pltpu.VMEM)),
        scratch_shapes=[
            pltpu.VMEM((piece * kv_width // LANES, LANES), jnp.float32), dma,
            pltpu.VMEM((rows, width), jnp.bfloat16),
            pltpu.VMEM((t, piece, width), jnp.bfloat16),
            pltpu.VMEM((t, blocks, LANES), jnp.float32),
            pltpu.VMEM((n * t, blocks, LANES), jnp.float32),
            dma((hops,)), dma((hops,)), dma((hops,)), dma((hops,)),
            dma((2 * hops + 2 * count,)), dma((2 * hops + 2 * count,)),
            dma((count,)), dma((count,)), dma, dma,
        ],
        compiler_params=pltpu.CompilerParams(
            collective_id=0, has_side_effects=True, vmem_limit_bytes=40 * 1024 * 1024),
    )(master_flat.reshape(piece * kv_width // LANES, LANES))
    out, scale = pl.pallas_call(
        store,
        out_shape=(jax.ShapeDtypeStruct(out.shape, out.dtype), jax.ShapeDtypeStruct(scale.shape, scale.dtype)),
        in_specs=[pl.BlockSpec(memory_space=pltpu.VMEM)] * 2,
        out_specs=(pl.BlockSpec(memory_space=pltpu.HBM),) * 2,
        scratch_shapes=[dma((PARTS,)), dma],
        compiler_params=pltpu.CompilerParams(vmem_limit_bytes=1024 * 1024),
    )(out, scale)
    return out.reshape(LAYERS, D, -1), scale.reshape(LAYERS, -1)


def solution(mesh):
    order = ring_order(mesh, mesh.shape["gx"] // CORES)
    in_specs = (P(("gx", "ta")),)
    out_specs = (P(None, None, "ta"), P(None, "ta"))
    return jax.shard_map(functools.partial(shards, mesh, order), mesh=mesh, in_specs=in_specs, out_specs=out_specs,
                         check_vma=False)
```
